512 devices in a mesh: dp: 32 (over y_hi, z), mp: 16 (over x, y_lo, core).
Axes of the slice: x: 4, y: 4 (y_hi: 2, y_lo: 2; y = y_hi * 2 + y_lo), z: 16, core: 2. Of those that a mesh axis runs over, the one named last changes fastest.
Arguments:
- tokens: bfloat16 [32768, 4096], P('dp', 'mp'), may hold values from -6 to 6
- right_weight: bfloat16 [64, 64, 64], P('mp', 'dp'), may hold values from -0.75 to 0.75
- left_weight: bfloat16 [64, 64, 64], P('mp', 'dp'), may hold values from -0.75 to 0.75
- cotangent: bfloat16 [32768, 4096], P('dp', 'mp'), may hold values from -0.032958984 to 0.032958984
Outputs:
- activated: bfloat16 [32768, 4096], P('dp', 'mp')
- grad_right: float32 [64, 64, 64], P('mp', 'dp')
- grad_left: float32 [64, 64, 64], P('mp', 'dp')
The draws below stay inside these ranges and needn't reach their ends.
All inputs are finite; a program needn't handle non-finite values.
Results may differ from the reference program's by a relative error of at most 0.0056.
Values may be sent and summed in bfloat16 or wider, within the bound.
No kernel may reach another device: no remote copies, remote signals or barrier semaphores. Data moves between devices by JAX's collectives and lax.ppermute only.
A program may use at most 64 MiB of HBM per device.

```python
import jax
import jax.numpy as jnp
from jax import lax

NB = 64
BS = 64
TOK_DEV = 1024
D = 4096
TOKENS = 32768
N_DP = 32


def block_scale(rng, dims, cuts, smallest, top_value):
    loudness, own = 1.0, jax.random.fold_in(rng, 6)
    for dim, shards_of in cuts:
        heights = jnp.exp(jax.random.uniform(jax.random.fold_in(own, dim), (shards_of,), jnp.float32, smallest / len(cuts), top_value / len(cuts)))
        loudness = loudness * jnp.repeat(heights, dims[dim] // shards_of).reshape([-1 if axis == dim else 1 for axis in range(len(dims))])
    return loudness


def scatter_about(rng, dims, width, limit, shards=(), dtype=jnp.bfloat16):
    result = width * jax.random.normal(rng, dims, jnp.float32)
    if shards:
        result = result * block_scale(rng, dims, shards, -0.22, 0.18)
    return jnp.clip(result, -limit, limit).astype(dtype)


def setup_inputs(seed: int = 0) -> dict:
    keys = jax.random.split(jax.random.key(seed), 5)
    return {
        "tokens": scatter_about(keys[0], (TOKENS, D), 1.0, 6.0, ((0, 32), (1, 16))),
        "right_weight": scatter_about(keys[1], (NB, BS, BS), BS ** -0.5, 0.75, ((0, 16), (1, 32))),
        "left_weight": scatter_about(keys[2], (BS, NB, BS), NB ** -0.5, 0.75, ((0, 16), (1, 32))),
        "cotangent": scatter_about(keys[3], (TOKENS, D), ((TOK_DEV * N_DP) ** -0.5), 0.032958984, ((0, 32), (1, 16))),
    }


def gelu_slope(pre):
    cdf = 0.5 * (1.0 + lax.erf(pre * 0.7071067811865476))
    density = jnp.exp(-0.5 * pre * pre) * 0.3989422804014327
    return cdf + pre * density


def reference(tokens, right_weight, left_weight, cotangent):
    right_f = right_weight.astype(jnp.float32)
    left_f = left_weight.astype(jnp.float32)
    xs_all = tokens.reshape(N_DP, TOK_DEV, NB, BS)
    gs_all = cotangent.reshape(N_DP, TOK_DEV, BS, BS)

    def step(carry, pieces):
        grad_r, grad_l = carry
        xs, gs = pieces
        xs_f = xs.astype(jnp.float32)
        inner = jnp.einsum('tik,ikm->tim', xs_f, right_f).astype(jnp.bfloat16)
        inner_f = inner.astype(jnp.float32)
        pre = jnp.einsum('tim,min->tmn', inner_f, left_f)
        activated = jax.nn.gelu(pre, approximate=False).astype(jnp.bfloat16)
        dpre = (gs.astype(jnp.float32) * gelu_slope(pre)).astype(jnp.bfloat16)
        dpre_f = dpre.astype(jnp.float32)
        grad_l = grad_l + jnp.einsum('tim,tmn->min', inner_f, dpre_f)
        dinner = jnp.einsum('tmn,min->tim', dpre_f, left_f).astype(jnp.bfloat16)
        grad_r = grad_r + jnp.einsum('tik,tim->ikm', xs_f, dinner.astype(jnp.float32))
        return (grad_r, grad_l), activated

    start = (jnp.zeros((NB, BS, BS), jnp.float32), jnp.zeros((BS, NB, BS), jnp.float32))
    (grad_right, grad_left), outs = lax.scan(step, start, (xs_all, gs_all))
    activated = outs.reshape(N_DP * TOK_DEV, NB * BS)
    return activated, grad_right, grad_left
```

```python
import jax
import jax.numpy as jnp
from jax import lax
from jax.sharding import PartitionSpec as P

NB = 64
BS = 64


def in_order(parts, dim):
    dims = list(parts.shape[1:])
    dims[dim] *= parts.shape[0]
    return jnp.moveaxis(parts, 0, dim).reshape(dims)


def gather_together(arrays, axis, dims):
    line = jnp.concatenate([a.reshape(-1) for a in arrays])
    devices = lax.axis_size(axis)
    copies = jnp.broadcast_to(line.reshape(1, -1, 128), (devices, line.size // 128, 128))
    lines = lax.all_to_all(copies, axis, 0, 0, tiled=True).reshape(devices, -1)
    at, gathered = (0, [])
    for a, dim in zip(arrays, dims):
        parts = lines[:, at : at + a.size].reshape(-1, *a.shape)
        gathered.append(in_order(parts, dim))
        at += a.size
    return tuple(gathered)


def cut_along(x, dim, devices):
    before, after = (x.shape[:dim], x.shape[dim + 1 :])
    return jnp.moveaxis(x.reshape(*before, devices, -1, *after), dim, 0)


def sent_and_summed(x, axis, dim):
    devices = lax.axis_size(axis)
    parts = lax.all_to_all(cut_along(x, dim, devices), axis, 0, 0, tiled=True)
    return jnp.sum(parts, axis=0)


def in_one_piece(arrays, axis, dim, along):
    widths = [a.shape[along] for a in arrays]
    both = jnp.concatenate(arrays, axis=along)
    result = sent_and_summed(both, axis, dim)
    return tuple(jnp.split(result, [sum(widths[:k]) for k in range(1, len(widths))], axis=along))


def gelu_slope(pre):
    cdf = 0.5 * (1.0 + lax.erf(pre * 0.7071067811865476))
    density = jnp.exp(-0.5 * pre * pre) * 0.3989422804014327
    return cdf + pre * density


def shards(tokens, right_weight, left_weight, cotangent):
    tok_rows = tokens.shape[0]
    groups = lax.axis_size("mp")
    owned = NB // groups
    right_rows, left_rows = gather_together((right_weight, left_weight), "dp", (1, 1))
    xs = tokens.reshape(tok_rows, owned, BS)
    inner = jnp.einsum("tik,ikm->tmi", xs, right_rows, preferred_element_type=jnp.float32)
    inner = inner.astype(jnp.bfloat16).reshape(tok_rows, BS * owned)
    left_four = left_rows.reshape(owned, groups, owned, BS)
    received = lax.all_to_all(inner, "mp", split_axis=1, concat_axis=1, tiled=True)
    rows = received.shape[0]
    mixed = received.reshape(rows, groups, owned, owned)
    pre_rows = jnp.einsum("tpmj,mpjn->tmn", mixed, left_four, preferred_element_type=jnp.float32)
    received, pre = (received, pre_rows)
    mixed = received.reshape(tok_rows, groups, owned, owned)
    activated = (
        jax.nn.gelu(pre, approximate=False).astype(jnp.bfloat16).reshape(tok_rows, owned * BS)
    )
    dpre = (cotangent.reshape(tok_rows, owned, BS).astype(jnp.float32) * gelu_slope(pre)).astype(
        jnp.bfloat16
    )
    part_left = jnp.einsum("tpmj,tmn->mpjn", mixed, dpre, preferred_element_type=jnp.float32)
    part_left = part_left.reshape(owned, NB, BS)
    dmixed = jnp.einsum("tmn,mpjn->tpmj", dpre, left_four, preferred_element_type=jnp.float32)
    dmixed = dmixed.astype(jnp.bfloat16).reshape(tok_rows, groups * owned * owned)
    dinner = lax.all_to_all(dmixed, "mp", split_axis=1, concat_axis=1, tiled=True)
    dinner = dinner.reshape(tok_rows, groups, owned, owned)
    part_right = jnp.einsum("tik,tqmi->ikqm", xs, dinner, preferred_element_type=jnp.float32)
    part_right = part_right.reshape(owned, BS, BS)
    grad_right, grad_left = in_one_piece((part_right, part_left), "dp", 1, 0)
    return (activated, grad_right, grad_left)


def solution(mesh):
    return jax.shard_map(
        shards,
        mesh=mesh,
        in_specs=(P("dp", "mp"), P("mp", "dp", None), P("mp", "dp", None), P("dp", "mp")),
        out_specs=(P("dp", "mp"), P("mp", "dp", None), P("mp", "dp", None)),
        check_vma=False,
    )
```

```python
import jax
import jax.numpy as jnp
import numpy as np
from jax import lax
from jax.sharding import PartitionSpec as P

NB = 64
BS = 64
F32, BF16 = jnp.float32, jnp.bfloat16
DP_FIRST = 24
MP_FIRST = 9


def order(size, first):
    return [(first + j) % size for j in range(size)]


def exchange(x, axis, members):
    return lax.all_to_all(x, axis, 0, 0, axis_index_groups=[members], tiled=True)


def dot(a, b, ca, cb):
    return lax.dot_general(a, b, (((ca,), (cb,)), ((), ())), preferred_element_type=F32)


def shards(tokens, right_weight, left_weight, cotangent):
    rows = tokens.shape[0]
    groups, n_dp = lax.axis_size("mp"), lax.axis_size("dp")
    owned, held = NB // groups, right_weight.shape[1]
    width = owned * BS
    dps, mps = order(n_dp, DP_FIRST % n_dp), order(groups, MP_FIRST % groups)

    mine = jnp.concatenate([right_weight, left_weight], axis=2)
    lines = exchange(jnp.broadcast_to(mine, (n_dp, *mine.shape)), "dp", dps)
    lines = jnp.roll(lines, dps[0], axis=0)
    right_rows = jnp.moveaxis(lines[..., :BS], 0, 1).reshape(width, BS)
    left_rows = jnp.moveaxis(lines[..., BS:], 0, 1).reshape(owned, NB, BS)

    column = np.arange(width)
    target = np.asarray(mps)[column // (owned * owned)] * owned + column % owned
    block = (column // owned) % owned
    spread = jnp.asarray(target)[None, :] == jnp.arange(BS)[:, None]
    own_block = jnp.arange(width)[:, None] // BS == jnp.asarray(block)[None, :]
    wide = dot(right_rows, spread.astype(BF16), 1, 0)
    right_wide = jnp.where(own_block, wide, 0.0).astype(BF16)

    inner = dot(right_wide, tokens, 0, 1).astype(BF16)
    inner = exchange(inner.reshape(groups, -1, rows), "mp", mps).reshape(width, rows)

    left_by_i = jnp.roll(jnp.moveaxis(left_rows, 1, 0), -mps[0] * owned, axis=0)
    eye = jnp.eye(owned, dtype=BF16)
    left_wide = (left_by_i[:, None] * eye[None, :, :, None]).reshape(width, width)

    pre = dot(inner, left_wide, 0, 0)
    cdf = 0.5 * (1.0 + lax.erf(pre * 0.7071067811865476))
    density = jnp.exp(-0.5 * pre * pre) * 0.3989422804014327
    activated = (pre * cdf).astype(BF16)
    dpre = (cotangent.astype(F32) * (cdf + pre * density)).astype(BF16)

    dmixed = dot(left_wide, dpre, 1, 1).astype(BF16)
    dinner = exchange(dmixed.reshape(groups, -1, rows), "mp", mps).reshape(width, rows)

    part_left = dot(inner, dpre, 1, 0).reshape(NB, owned, owned, BS)
    part_left = jnp.sum(part_left * eye.astype(F32)[None, :, :, None], axis=2).astype(BF16)
    part_left = jnp.roll(part_left, mps[0] * owned, axis=0)
    part_left = part_left.reshape(n_dp, held, owned, BS).swapaxes(1, 2)

    part_right = dot(tokens, dinner, 0, 1)
    part_right = jnp.where(own_block, part_right, 0.0).astype(BF16)
    part_right = dot(part_right, spread.astype(BF16), 1, 1).astype(BF16)
    part_right = jnp.moveaxis(part_right.reshape(owned, n_dp, held, BS), 1, 0)

    parts = jnp.roll(jnp.concatenate([part_right, part_left], axis=3), -dps[0], axis=0)
    sums = jnp.sum(exchange(parts, "dp", dps).astype(F32), axis=0)
    return (activated, sums[..., :BS], sums[..., BS:])


def solution(mesh):
    return jax.shard_map(
        shards,
        mesh=mesh,
        in_specs=(P("dp", "mp"), P("mp", "dp", None), P("mp", "dp", None), P("dp", "mp")),
        out_specs=(P("dp", "mp"), P("mp", "dp", None), P("mp", "dp", None)),
        check_vma=False,
    )
```

```python
import functools

import jax
import jax.numpy as jnp
from jax import lax
from jax.experimental import pallas as pl
from jax.experimental.pallas import tpu as pltpu
from jax.sharding import PartitionSpec as P

NB = 64
BS = 64
F32, BF16 = jnp.float32, jnp.bfloat16
DP_FIRST = 24
MP_FIRST = 9
STEP = 256


def exchange(x, axis, first):
    size = lax.axis_size(axis)
    members = [(first + j) % size for j in range(size)]
    return lax.all_to_all(x, axis, 0, 0, axis_index_groups=[members], tiled=True)


def dot(a, b, ca, cb):
    return lax.dot_general(a, b, (((ca,), (cb,)), ((), ())), preferred_element_type=F32)


def where(rows, columns, test):
    r = lax.broadcasted_iota(jnp.int32, (rows, columns), 0)
    c = lax.broadcasted_iota(jnp.int32, (rows, columns), 1)
    return test(r, c)


def one_hot(rows, columns, test):
    return jnp.where(where(rows, columns, test), 1.0, 0.0).astype(BF16)


class Plan:
    def __init__(self, groups, n_dp, held):
        self.groups, self.n_dp, self.held = groups, n_dp, held
        self.owned = NB // groups
        self.width = self.owned * BS

    def peer_m(self, r):
        return r // self.held % self.owned

    def peer_i(self, r):
        chunk = self.owned * self.owned
        return r % chunk // (self.owned * self.held) * self.held + r % self.held

    def target(self, r):
        peer = (r // (self.owned * self.owned) + MP_FIRST) % self.groups
        return peer * self.owned + self.peer_m(r)

    def line_feature(self, r):
        line = self.owned * self.held
        member = (r // line + DP_FIRST) % self.n_dp
        return r % line // self.held * BS + member * self.held + r % self.held

    def spread(self):
        return one_hot(self.width, 2 * BS, lambda r, c: self.target(r) == c)

    def features(self):
        return one_hot(self.width, self.width, lambda r, c: self.line_feature(r) == c)

    def own_block(self, x):
        own = where(self.width, self.width, lambda r, c: self.peer_i(r) == c // BS)
        return jnp.where(own, x, 0.0).astype(BF16)

    def tiles(self):
        return one_hot(2 * BS, self.width, lambda n, c: n == c % BS + BS)

    def own_m(self, x):
        own = where(self.width, self.width, lambda r, c: self.peer_m(r) == c // BS)
        return jnp.where(own, x, 0.0).astype(BF16)

    def turn(self, x, back):
        line = self.owned * self.held
        by = (MP_FIRST * self.owned * self.owned - DP_FIRST * line) % self.width
        by = self.width - by if back else by
        return jnp.concatenate([x[by:], x[:by]], axis=0) if by else x


def first_kernel(plan, lines, tokens, inner):
    right = dot(plan.spread(), lines[...], 1, 1).astype(BF16)
    right = plan.own_block(dot(right, plan.features(), 1, 0))
    inner[...] = dot(right, tokens[...], 1, 1).astype(BF16)


def middle_kernel(plan, lines, inner, cotangent, dmixed, part_left, activated, act, sems):
    left = plan.own_m(dot(plan.turn(lines[...], False), plan.tiles(), 1, 0))
    steps = inner.shape[1] // STEP
    total = None
    copies = []
    for s in range(steps):
        at = pl.ds(s * STEP, STEP)
        some = inner[:, at]
        pre = dot(some, left, 0, 0)
        cdf = 0.5 * (1.0 + lax.erf(pre * 0.7071067811865476))
        density = jnp.exp(-0.5 * pre * pre) * 0.3989422804014327
        act[at, :] = (pre * cdf).astype(BF16)
        copies.append(pltpu.make_async_copy(act.at[at, :], activated.at[at, :], sems.at[s]))
        copies[-1].start()
        dpre = (cotangent[at, :].astype(F32) * (cdf + pre * density)).astype(BF16)
        dmixed[:, at] = dot(left, dpre, 1, 1).astype(BF16)
        part = dot(some, dpre, 1, 0)
        total = part if total is None else total + part
    part_left[...] = plan.turn(dot(plan.own_m(total), plan.tiles(), 1, 1), True).astype(BF16)
    for copy in copies:
        copy.wait()


def last_kernel(plan, dinner, tokens, part_left, parts):
    part = plan.own_block(dot(dinner[...], tokens[...], 1, 0))
    part = dot(plan.spread(), part, 0, 0).astype(BF16)
    parts[...] = (dot(plan.features(), part, 1, 1) + part_left[...].astype(F32)).astype(BF16)


VMEM = pl.BlockSpec(memory_space=pltpu.VMEM)
PARAMS = pltpu.CompilerParams(vmem_limit_bytes=24 * 1024 * 1024)


def shards(tokens, right_weight, left_weight, cotangent):
    rows = tokens.shape[0]
    groups, n_dp = lax.axis_size("mp"), lax.axis_size("dp")
    plan = Plan(groups, n_dp, right_weight.shape[1])
    width = plan.width

    mine = jnp.concatenate([right_weight, left_weight], axis=2)
    lines = exchange(jnp.broadcast_to(mine, (n_dp, *mine.shape)), "dp", DP_FIRST)
    lines = lines.reshape(width, 2 * BS)

    inner = pl.pallas_call(
        functools.partial(first_kernel, plan),
        out_shape=jax.ShapeDtypeStruct((width, rows), BF16),
        in_specs=[VMEM] * 2,
        out_specs=VMEM,
        compiler_params=PARAMS,
    )(lines, tokens)
    inner = exchange(inner.reshape(groups, -1, rows), "mp", MP_FIRST).reshape(width, rows)

    dmixed, part_left, activated = pl.pallas_call(
        functools.partial(middle_kernel, plan),
        out_shape=(
            jax.ShapeDtypeStruct((width, rows), BF16),
            jax.ShapeDtypeStruct((width, 2 * BS), BF16),
            jax.ShapeDtypeStruct((rows, width), BF16),
        ),
        in_specs=[VMEM] * 3,
        out_specs=(VMEM, VMEM, pl.BlockSpec(memory_space=pl.ANY)),
        scratch_shapes=[pltpu.VMEM((rows, width), BF16), pltpu.SemaphoreType.DMA((rows // STEP,))],
        compiler_params=PARAMS,
    )(lines, inner, cotangent)
    dinner = exchange(dmixed.reshape(groups, -1, rows), "mp", MP_FIRST).reshape(width, rows)

    parts = pl.pallas_call(
        functools.partial(last_kernel, plan),
        out_shape=jax.ShapeDtypeStruct((width, 2 * BS), BF16),
        in_specs=[VMEM] * 3,
        out_specs=VMEM,
        compiler_params=PARAMS,
    )(dinner, tokens, part_left)
    sums = jnp.sum(exchange(parts.reshape(n_dp, *mine.shape), "dp", DP_FIRST).astype(F32), axis=0)
    return (activated, sums[..., :BS], sums[..., BS:])


def solution(mesh):
    return jax.shard_map(
        shards,
        mesh=mesh,
        in_specs=(P("dp", "mp"), P("mp", "dp", None), P("mp", "dp", None), P("dp", "mp")),
        out_specs=(P("dp", "mp"), P("mp", "dp", None), P("mp", "dp", None)),
        check_vma=False,
    )
```

```python
import functools

import jax
import jax.numpy as jnp
from jax import lax
from jax.experimental import pallas as pl
from jax.experimental.pallas import tpu as pltpu
from jax.sharding import PartitionSpec as P

NB = 64
BS = 64
F32, BF16 = jnp.float32, jnp.bfloat16
DP_FIRST = 24
MP_FIRST = 9
STEP = 256


def exchange(x, axis, first):
    size = lax.axis_size(axis)
    members = [(first + j) % size for j in range(size)]
    return lax.all_to_all(x, axis, 0, 0, axis_index_groups=[members], tiled=True)


def dot(a, b, ca, cb):
    return lax.dot_general(a, b, (((ca,), (cb,)), ((), ())), preferred_element_type=F32)


def div(x, n):
    return lax.shift_right_logical(x, jnp.int32(n.bit_length() - 1))


def mod(x, n):
    return x & (n - 1)


def equal(rows, columns, of_row, of_column):
    r = of_row(lax.broadcasted_iota(jnp.int32, (rows, 128), 0))
    c = of_column(lax.broadcasted_iota(jnp.int32, (1, columns), 1))
    return jnp.concatenate([r] * (columns // 128), axis=1) == c


def one_hot(rows, columns, of_row, of_column):
    return jnp.where(equal(rows, columns, of_row, of_column), 1.0, 0.0).astype(BF16)


class Plan:
    def __init__(self, groups, n_dp, held):
        self.groups, self.n_dp, self.held = groups, n_dp, held
        self.owned = NB // groups
        self.width = self.owned * BS
        assert all(n & (n - 1) == 0 for n in (groups, n_dp, held))

    def peer_m(self, r):
        return mod(div(r, self.held), self.owned)

    def peer_i(self, r):
        high = div(mod(r, self.owned * self.owned), self.owned * self.held)
        return high * self.held + mod(r, self.held)

    def target(self, r):
        peer = mod(div(r, self.owned * self.owned) + MP_FIRST, self.groups)
        return peer * self.owned + self.peer_m(r)

    def line_feature(self, r):
        line = self.owned * self.held
        member = mod(div(r, line) + DP_FIRST, self.n_dp)
        return div(mod(r, line), self.held) * BS + member * self.held + mod(r, self.held)

    def spread(self):
        return one_hot(self.width, 2 * BS, self.target, lambda c: c)

    def features(self):
        return one_hot(self.width, self.width, self.line_feature, lambda c: c)

    def own_block(self, x):
        own = equal(self.width, self.width, self.peer_i, lambda c: div(c, BS))
        return jnp.where(own, x, 0.0).astype(BF16)

    def tiles(self):
        return one_hot(2 * BS, self.width, lambda n: n, lambda c: mod(c, BS) + BS)

    def own_m(self, x):
        own = equal(self.width, self.width, self.peer_m, lambda c: div(c, BS))
        return jnp.where(own, x, 0.0).astype(BF16)

    def turn(self, x, back):
        line = self.owned * self.held
        by = (MP_FIRST * self.owned * self.owned - DP_FIRST * line) % self.width
        by = self.width - by if back else by
        return jnp.concatenate([x[by:], x[:by]], axis=0) if by else x


def load_kernel(right, left, tokens, copies, held, r, l, sems):
    loads = [
        pltpu.make_async_copy(a, b, sems.at[k])
        for k, (a, b) in enumerate(((right, r), (left, l), (tokens, held)))
    ]
    for load in loads:
        load.start()
    loads[0].wait()
    loads[1].wait()
    copies[...] = jnp.broadcast_to(jnp.concatenate([r[...], l[...]], axis=2), copies.shape)
    loads[2].wait()


def first_kernel(plan, lines, tokens, inner):
    right = dot(plan.spread(), lines[...], 1, 1).astype(BF16)
    right = plan.own_block(dot(right, plan.features(), 1, 0))
    inner[...] = dot(right, tokens[...], 1, 1).astype(BF16)


def middle_kernel(plan, lines, inner, cotangent, dmixed, part_left, activated, act, sems):
    left = plan.own_m(dot(plan.turn(lines[...], False), plan.tiles(), 1, 0))
    steps = inner.shape[1] // STEP
    copies, dpres = [], []
    for s in range(steps):
        at = pl.ds(s * STEP, STEP)
        pre = dot(inner[:, at], left, 0, 0)
        cdf = 0.5 * (1.0 + lax.erf(pre * 0.7071067811865476))
        density = jnp.exp(-0.5 * pre * pre) * 0.3989422804014327
        act[at, :] = (pre * cdf).astype(BF16)
        copies.append(pltpu.make_async_copy(act.at[at, :], activated.at[at, :], sems.at[s]))
        copies[-1].start()
        slope = cdf + pre * density
        dpres.append((cotangent[at, :].astype(F32) * slope).astype(BF16))
    dpre = jnp.concatenate(dpres, axis=0)
    dmixed[...] = dot(left, dpre, 1, 1).astype(BF16)
    total = dot(inner[...], dpre, 1, 0)
    part_left[...] = plan.turn(dot(plan.own_m(total), plan.tiles(), 1, 1), True).astype(BF16)
    for copy in copies:
        copy.wait()


def last_kernel(plan, dinner, tokens, part_left, parts):
    part = plan.own_block(dot(dinner[...], tokens[...], 1, 0))
    part = dot(plan.spread(), part, 0, 0).astype(BF16)
    parts[...] = (dot(plan.features(), part, 1, 1) + part_left[...].astype(F32)).astype(BF16)


HBM = pl.BlockSpec(memory_space=pltpu.HBM)
VMEM = pl.BlockSpec(memory_space=pltpu.VMEM)
PARAMS = pltpu.CompilerParams(vmem_limit_bytes=24 * 1024 * 1024)


def shards(tokens, right_weight, left_weight, cotangent):
    rows = tokens.shape[0]
    groups, n_dp = lax.axis_size("mp"), lax.axis_size("dp")
    plan = Plan(groups, n_dp, right_weight.shape[1])
    width = plan.width

    line = (*right_weight.shape[:2], 2 * BS)
    copies, tokens = pl.pallas_call(
        load_kernel,
        out_shape=(
            pltpu.VMEM((n_dp, *line), BF16),
            pltpu.VMEM(tokens.shape, BF16),
        ),
        in_specs=[HBM] * 3,
        out_specs=(VMEM, VMEM),
        scratch_shapes=[
            pltpu.VMEM(right_weight.shape, BF16),
            pltpu.VMEM(left_weight.shape, BF16),
            pltpu.SemaphoreType.DMA((3,)),
        ],
        compiler_params=pltpu.CompilerParams(vmem_limit_bytes=60 * 1024 * 1024),
    )(right_weight, left_weight, tokens)
    lines = exchange(copies, "dp", DP_FIRST)
    lines = lines.reshape(width, 2 * BS)

    inner = pl.pallas_call(
        functools.partial(first_kernel, plan),
        out_shape=jax.ShapeDtypeStruct((width, rows), BF16),
        in_specs=[VMEM] * 2,
        out_specs=VMEM,
        compiler_params=PARAMS,
    )(lines, tokens)
    inner = exchange(inner.reshape(groups, -1, rows), "mp", MP_FIRST).reshape(width, rows)

    dmixed, part_left, activated = pl.pallas_call(
        functools.partial(middle_kernel, plan),
        out_shape=(
            jax.ShapeDtypeStruct((width, rows), BF16),
            jax.ShapeDtypeStruct((width, 2 * BS), BF16),
            jax.ShapeDtypeStruct((rows, width), BF16),
        ),
        in_specs=[VMEM] * 3,
        out_specs=(VMEM, VMEM, HBM),
        scratch_shapes=[pltpu.VMEM((rows, width), BF16), pltpu.SemaphoreType.DMA((rows // STEP,))],
        compiler_params=PARAMS,
    )(lines, inner, cotangent)
    dinner = exchange(dmixed.reshape(groups, -1, rows), "mp", MP_FIRST).reshape(width, rows)

    parts = pl.pallas_call(
        functools.partial(last_kernel, plan),
        out_shape=jax.ShapeDtypeStruct((width, 2 * BS), BF16),
        in_specs=[VMEM] * 3,
        out_specs=VMEM,
        compiler_params=PARAMS,
    )(dinner, tokens, part_left)
    sums = jnp.sum(exchange(parts.reshape(n_dp, *line), "dp", DP_FIRST).astype(F32), axis=0)
    return (activated, sums[..., :BS], sums[..., BS:])


def solution(mesh):
    return jax.shard_map(
        shards,
        mesh=mesh,
        in_specs=(P("dp", "mp"), P("mp", "dp", None), P("mp", "dp", None), P("dp", "mp")),
        out_specs=(P("dp", "mp"), P("mp", "dp", None), P("mp", "dp", None)),
        check_vma=False,
    )
```

```python
import functools

import jax
import jax.numpy as jnp
from jax import lax
from jax.experimental import pallas as pl
from jax.experimental.pallas import tpu as pltpu
from jax.sharding import PartitionSpec as P

NB = 64
BS = 64
F32, BF16 = jnp.float32, jnp.bfloat16
WEIGHTS_FIRST = 26
GRADS_FIRST = 24
MP_FIRST = 9
STEPS = (256, 512, 256)


def exchange(x, axis, first):
    size = lax.axis_size(axis)
    members = [(first + j) % size for j in range(size)]
    return lax.all_to_all(x, axis, 0, 0, axis_index_groups=[members], tiled=True)


def dot(a, b, ca, cb):
    return lax.dot_general(a, b, (((ca,), (cb,)), ((), ())), preferred_element_type=F32)


def div(x, n):
    return lax.shift_right_logical(x, jnp.int32(n.bit_length() - 1))


def mod(x, n):
    return x & (n - 1)


def one_hot(ref, of_row, of_column):
    rows, columns = ref.shape
    r = of_row(lax.broadcasted_iota(jnp.int32, (rows, 128), 0))
    c = of_column(lax.broadcasted_iota(jnp.int32, (1, columns), 1))
    same = jnp.concatenate([r] * (columns // 128), axis=1) == c
    ref[...] = jnp.where(same, 1.0, 0.0).astype(BF16)


class Plan:
    def __init__(self, groups, n_dp, held):
        self.groups, self.n_dp, self.held = groups, n_dp, held
        self.owned = NB // groups
        self.width = self.owned * BS
        self.line = self.owned * held
        assert all(n & (n - 1) == 0 for n in (groups, n_dp, held))

    def peer_m(self, r):
        return mod(div(r, self.held), self.owned)

    def peer_i(self, r):
        high = div(mod(r, self.owned * self.owned), self.line)
        return high * self.held + mod(r, self.held)

    def target(self, r):
        peer = mod(div(r, self.owned * self.owned) + MP_FIRST, self.groups)
        return peer * self.owned + self.peer_m(r)

    def feature(self, r, first):
        member = mod(div(r, self.line) + first, self.n_dp)
        return div(mod(r, self.line), self.held) * BS + member * self.held + mod(r, self.held)

    def turn(self, x, first, back):
        by = (MP_FIRST * self.owned * self.owned - first * self.line) % self.width
        by = self.width - by if back else by
        return jnp.concatenate([x[by:], x[:by]], axis=0) if by % self.width else x


def load_kernel(
    plan, right, left, tokens, copies, held, spread, unspread, tiles, wfeatures, gfeatures, block, m, r, l, sems
):
    rows = tokens.shape[0] // 4
    loads = [pltpu.make_async_copy(right, r, sems.at[0]), pltpu.make_async_copy(left, l, sems.at[1])]
    for k in range(4):
        at = pl.ds(k * rows, rows)
        loads.append(pltpu.make_async_copy(tokens.at[at, :], held.at[at, :], sems.at[2 + k]))
    for load in loads:
        load.start()
    one_hot(spread, plan.target, lambda c: c)
    one_hot(unspread, lambda n: n, plan.target)
    one_hot(tiles, lambda n: n, lambda c: mod(c, BS) + BS)
    one_hot(wfeatures, lambda n: plan.feature(n, WEIGHTS_FIRST), lambda c: c)
    one_hot(gfeatures, lambda n: plan.feature(n, GRADS_FIRST), lambda c: c)
    one_hot(block, plan.peer_i, lambda c: div(c, BS))
    one_hot(m, plan.peer_m, lambda c: div(c, BS))
    loads[0].wait()
    loads[1].wait()
    copies[...] = jnp.broadcast_to(jnp.concatenate([r[...], l[...]], axis=2), copies.shape)
    for load in loads[2:]:
        load.wait()


def first_kernel(plan, lines, tokens, spread, tiles, features, block, m, inner, left):
    right = dot(spread[...], lines[...], 1, 1).astype(BF16)
    right = dot(right, features[...], 1, 0).astype(BF16) * block[...]
    inner[...] = dot(right, tokens[...], 1, 1).astype(BF16)
    turned = plan.turn(lines[...], WEIGHTS_FIRST, False)
    left[...] = (dot(turned, tiles[...], 1, 0) * 0.5).astype(BF16) * m[...]


def middle_kernel(plan, left, inner, cotangent, tiles, m, dmixed, part_left, activated, act, pres, dpres, sems):
    steps, copies = len(STEPS), []
    spans = [pl.ds(sum(STEPS[:s]), STEPS[s]) for s in range(steps)]

    def pre_of(s):
        pres[spans[s], :] = dot(inner[:, spans[s]], left[...], 0, 0)

    def slope_of(s):
        at = spans[s]
        half = pres[at, :]
        twice_cdf = 1.0 + lax.erf(half * 1.4142135623730951)
        act[at, :] = (half * twice_cdf).astype(BF16)
        density = jnp.exp2(half * half * -2.8853900817779268) * 1.5957691216057308
        slope = twice_cdf + half * density
        dpres[at, :] = (cotangent[at, :].astype(F32) * slope).astype(BF16)

    def products_of(s, total):
        at = spans[s]
        dmixed[:, at] = dot(left[...], dpres[at, :], 1, 1).astype(BF16)
        part = dot(inner[:, at], dpres[at, :], 1, 0)
        return part if total is None else total + part

    total = None
    pre_of(0)
    for s in range(steps):
        if s + 1 < steps:
            pre_of(s + 1)
        slope_of(s)
        if s:
            total = products_of(s - 1, total)
        at = spans[s]
        copies.append(pltpu.make_async_copy(act.at[at, :], activated.at[at, :], sems.at[s]))
        copies[-1].start()
    total = products_of(steps - 1, total)
    part = (total * 0.5).astype(BF16) * m[...]
    part_left[...] = plan.turn(dot(part, tiles[...], 1, 1), GRADS_FIRST, True).astype(BF16)
    for copy in copies:
        copy.wait()


def last_kernel(plan, dinner, tokens, part_left, unspread, features, block, parts):
    part = dot(dinner[...], tokens[...], 1, 0).astype(BF16) * block[...]
    part = dot(unspread[...], part, 1, 0).astype(BF16)
    parts[...] = (dot(features[...], part, 1, 1) + part_left[...].astype(F32)).astype(BF16)


HBM = pl.BlockSpec(memory_space=pltpu.HBM)
VMEM = pl.BlockSpec(memory_space=pltpu.VMEM)


def call(kernel, inputs, outputs, scratch=(), hbm_in=False, hbm_out=(), limit=24):
    outs = tuple(
        jax.ShapeDtypeStruct(shape, BF16) if k in hbm_out else pltpu.VMEM(shape, BF16)
        for k, shape in enumerate(outputs)
    )
    return pl.pallas_call(
        kernel,
        out_shape=outs,
        in_specs=[HBM if hbm_in else VMEM] * len(inputs),
        out_specs=tuple(HBM if k in hbm_out else VMEM for k in range(len(outs))),
        scratch_shapes=scratch,
        compiler_params=pltpu.CompilerParams(vmem_limit_bytes=limit * 1024 * 1024),
    )(*inputs)


def shards(tokens, right_weight, left_weight, cotangent):
    rows = tokens.shape[0]
    groups, n_dp = lax.axis_size("mp"), lax.axis_size("dp")
    plan = Plan(groups, n_dp, right_weight.shape[1])
    width = plan.width
    line = (*right_weight.shape[:2], 2 * BS)
    square, tall, wide = (width, width), (width, 2 * BS), (2 * BS, width)

    copies, tokens, spread, unspread, tiles, wfeatures, gfeatures, block, m = call(
        functools.partial(load_kernel, plan),
        (right_weight, left_weight, tokens),
        ((n_dp, *line), tokens.shape, tall, wide, wide, square, square, square, square),
        scratch=[
            pltpu.VMEM(right_weight.shape, BF16),
            pltpu.VMEM(left_weight.shape, BF16),
            pltpu.SemaphoreType.DMA((6,)),
        ],
        hbm_in=True,
        limit=60,
    )
    lines = exchange(copies, "dp", WEIGHTS_FIRST).reshape(tall)

    inner, left = call(
        functools.partial(first_kernel, plan),
        (lines, tokens, spread, tiles, wfeatures, block, m),
        ((width, rows), square),
    )
    inner = exchange(inner.reshape(groups, -1, rows), "mp", MP_FIRST).reshape(width, rows)

    dmixed, part_left, activated = call(
        functools.partial(middle_kernel, plan),
        (left, inner, cotangent, tiles, m),
        ((width, rows), tall, (rows, width)),
        scratch=[
            pltpu.VMEM((rows, width), BF16),
            pltpu.VMEM((rows, width), F32),
            pltpu.VMEM((rows, width), BF16),
            pltpu.SemaphoreType.DMA((len(STEPS),)),
        ],
        hbm_out=(2,),
    )
    dinner = exchange(dmixed.reshape(groups, -1, rows), "mp", MP_FIRST).reshape(width, rows)

    (parts,) = call(
        functools.partial(last_kernel, plan),
        (dinner, tokens, part_left, unspread, gfeatures, block),
        (tall,),
    )
    sums = jnp.sum(exchange(parts.reshape(n_dp, *line), "dp", GRADS_FIRST).astype(F32), axis=0)
    return (activated, sums[..., :BS], sums[..., BS:])


def solution(mesh):
    return jax.shard_map(
        shards,
        mesh=mesh,
        in_specs=(P("dp", "mp"), P("mp", "dp", None), P("mp", "dp", None), P("dp", "mp")),
        out_specs=(P("dp", "mp"), P("mp", "dp", None), P("mp", "dp", None)),
        check_vma=False,
    )
```

```python
import functools

import jax
import jax.numpy as jnp
from jax import lax
from jax.experimental import pallas as pl
from jax.experimental.pallas import tpu as pltpu
from jax.sharding import PartitionSpec as P

NB = 64
BS = 64
F32, BF16 = jnp.float32, jnp.bfloat16
WEIGHTS_FIRST = 26
GRADS_FIRST = 24
MP_FIRST = 9
STEPS = (256, 512, 256)


def exchange(x, axis, first):
    size = lax.axis_size(axis)
    members = [(first + j) % size for j in range(size)]
    return lax.all_to_all(x, axis, 0, 0, axis_index_groups=[members], tiled=True)


def dot(a, b, ca, cb):
    return lax.dot_general(a, b, (((ca,), (cb,)), ((), ())), preferred_element_type=F32)


def div(x, n):
    return lax.shift_right_logical(x, jnp.int32(n.bit_length() - 1))


def mod(x, n):
    return x & (n - 1)


def one_hot(ref, of_row, of_column):
    rows, columns = ref.shape
    r = of_row(lax.broadcasted_iota(jnp.int32, (rows, 128), 0))
    c = of_column(lax.broadcasted_iota(jnp.int32, (1, columns), 1))
    same = jnp.concatenate([r] * (columns // 128), axis=1) == c
    ref[...] = jnp.where(same, 1.0, 0.0).astype(BF16)


class Plan:
    def __init__(self, groups, n_dp, held):
        self.groups, self.n_dp, self.held = groups, n_dp, held
        self.owned = NB // groups
        self.width = self.owned * BS
        self.line = self.owned * held
        assert all(n & (n - 1) == 0 for n in (groups, n_dp, held))

    def peer_m(self, r):
        return mod(div(r, self.held), self.owned)

    def peer_i(self, r):
        high = div(mod(r, self.owned * self.owned), self.line)
        return high * self.held + mod(r, self.held)

    def target(self, r):
        peer = mod(div(r, self.owned * self.owned) + MP_FIRST, self.groups)
        return peer * self.owned + self.peer_m(r)

    def feature(self, r, first):
        member = mod(div(r, self.line) + first, self.n_dp)
        return div(mod(r, self.line), self.held) * BS + member * self.held + mod(r, self.held)

    def turn(self, x, first, back):
        by = (MP_FIRST * self.owned * self.owned - first * self.line) % self.width
        by = self.width - by if back else by
        return jnp.concatenate([x[by:], x[:by]], axis=0) if by % self.width else x


def load_kernel(plan, right, left, copies, spread, unspread, tiles, wfeatures, gfeatures, block, m, r, l, sems):
    loads = [pltpu.make_async_copy(right, r, sems.at[0]), pltpu.make_async_copy(left, l, sems.at[1])]
    for load in loads:
        load.start()
    one_hot(spread, plan.target, lambda c: c)
    one_hot(unspread, lambda n: n, plan.target)
    one_hot(tiles, lambda n: n, lambda c: mod(c, BS) + BS)
    one_hot(wfeatures, lambda n: plan.feature(n, WEIGHTS_FIRST), lambda c: c)
    one_hot(gfeatures, lambda n: plan.feature(n, GRADS_FIRST), lambda c: c)
    one_hot(block, plan.peer_i, lambda c: div(c, BS))
    one_hot(m, plan.peer_m, lambda c: div(c, BS))
    for load in loads:
        load.wait()
    copies[...] = jnp.broadcast_to(jnp.concatenate([r[...], l[...]], axis=2), copies.shape)


def first_kernel(plan, lines, spread, tiles, features, block, m, right, left):
    some = dot(spread[...], lines[...], 1, 1).astype(BF16)
    right[...] = dot(some, features[...], 1, 0).astype(BF16) * block[...]
    turned = plan.turn(lines[...], WEIGHTS_FIRST, False)
    left[...] = (dot(turned, tiles[...], 1, 0) * 0.5).astype(BF16) * m[...]


def middle_kernel(plan, left, inner, cotangent, tiles, m, dmixed, part_left, activated, act, pres, dpres, sems):
    steps, copies = len(STEPS), []
    spans = [pl.ds(sum(STEPS[:s]), STEPS[s]) for s in range(steps)]

    def pre_of(s):
        pres[spans[s], :] = dot(inner[:, spans[s]], left[...], 0, 0)

    def slope_of(s):
        at = spans[s]
        half = pres[at, :]
        twice_cdf = 1.0 + lax.erf(half * 1.4142135623730951)
        act[at, :] = (half * twice_cdf).astype(BF16)
        density = jnp.exp2(half * half * -2.8853900817779268) * 1.5957691216057308
        slope = twice_cdf + half * density
        dpres[at, :] = (cotangent[at, :].astype(F32) * slope).astype(BF16)

    def products_of(s, total):
        at = spans[s]
        dmixed[:, at] = dot(left[...], dpres[at, :], 1, 1).astype(BF16)
        part = dot(inner[:, at], dpres[at, :], 1, 0)
        return part if total is None else total + part

    total = None
    pre_of(0)
    for s in range(steps):
        if s + 1 < steps:
            pre_of(s + 1)
        slope_of(s)
        if s:
            total = products_of(s - 1, total)
        at = spans[s]
        copies.append(pltpu.make_async_copy(act.at[at, :], activated.at[at, :], sems.at[s]))
        copies[-1].start()
    total = products_of(steps - 1, total)
    part = (total * 0.5).astype(BF16) * m[...]
    part_left[...] = plan.turn(dot(part, tiles[...], 1, 1), GRADS_FIRST, True).astype(BF16)
    for copy in copies:
        copy.wait()


def last_kernel(plan, part, part_left, unspread, features, parts):
    part = dot(unspread[...], part[...], 1, 0).astype(BF16)
    parts[...] = (dot(features[...], part, 1, 1) + part_left[...].astype(F32)).astype(BF16)


HBM = pl.BlockSpec(memory_space=pltpu.HBM)
VMEM = pl.BlockSpec(memory_space=pltpu.VMEM)


def call(kernel, inputs, outputs, scratch=(), hbm_in=False, hbm_out=(), limit=24):
    outs = tuple(
        jax.ShapeDtypeStruct(shape, BF16) if k in hbm_out else pltpu.VMEM(shape, BF16)
        for k, shape in enumerate(outputs)
    )
    return pl.pallas_call(
        kernel,
        out_shape=outs,
        in_specs=[HBM if hbm_in else VMEM] * len(inputs),
        out_specs=tuple(HBM if k in hbm_out else VMEM for k in range(len(outs))),
        scratch_shapes=scratch,
        compiler_params=pltpu.CompilerParams(vmem_limit_bytes=limit * 1024 * 1024),
    )(*inputs)


def shards(tokens, right_weight, left_weight, cotangent):
    rows = tokens.shape[0]
    groups, n_dp = lax.axis_size("mp"), lax.axis_size("dp")
    plan = Plan(groups, n_dp, right_weight.shape[1])
    width = plan.width
    line = (*right_weight.shape[:2], 2 * BS)
    square, tall, wide = (width, width), (width, 2 * BS), (2 * BS, width)

    copies, spread, unspread, tiles, wfeatures, gfeatures, block, m = call(
        functools.partial(load_kernel, plan),
        (right_weight, left_weight),
        ((n_dp, *line), tall, wide, wide, square, square, square, square),
        scratch=[
            pltpu.VMEM(right_weight.shape, BF16),
            pltpu.VMEM(left_weight.shape, BF16),
            pltpu.SemaphoreType.DMA((2,)),
        ],
        hbm_in=True,
        limit=60,
    )
    lines = exchange(copies, "dp", WEIGHTS_FIRST).reshape(tall)

    right, left = call(
        functools.partial(first_kernel, plan),
        (lines, spread, tiles, wfeatures, block, m),
        (square, square),
    )
    inner = dot(right, tokens, 1, 1).astype(BF16)
    inner = exchange(inner.reshape(groups, -1, rows), "mp", MP_FIRST).reshape(width, rows)

    dmixed, part_left, activated = call(
        functools.partial(middle_kernel, plan),
        (left, inner, cotangent, tiles, m),
        ((width, rows), tall, (rows, width)),
        scratch=[
            pltpu.VMEM((rows, width), BF16),
            pltpu.VMEM((rows, width), F32),
            pltpu.VMEM((rows, width), BF16),
            pltpu.SemaphoreType.DMA((len(STEPS),)),
        ],
        hbm_out=(2,),
    )
    dinner = exchange(dmixed.reshape(groups, -1, rows), "mp", MP_FIRST).reshape(width, rows)

    part = dot(dinner, tokens, 1, 0).astype(BF16) * block
    (parts,) = call(
        functools.partial(last_kernel, plan),
        (part, part_left, unspread, gfeatures),
        (tall,),
    )
    sums = jnp.sum(exchange(parts.reshape(n_dp, *line), "dp", GRADS_FIRST).astype(F32), axis=0)
    return (activated, sums[..., :BS], sums[..., BS:])


def solution(mesh):
    return jax.shard_map(
        shards,
        mesh=mesh,
        in_specs=(P("dp", "mp"), P("mp", "dp", None), P("mp", "dp", None), P("dp", "mp")),
        out_specs=(P("dp", "mp"), P("mp", "dp", None), P("mp", "dp", None)),
        check_vma=False,
    )
```

```python
import functools

import jax
import jax.numpy as jnp
from jax import lax
from jax.experimental import pallas as pl
from jax.experimental.pallas import tpu as pltpu
from jax.sharding import PartitionSpec as P

NB = 64
BS = 64
F32, BF16 = jnp.float32, jnp.bfloat16
DP_FIRST = 24
MP_FIRST = 9
STEPS = (256, 512, 256)


def exchange(x, axis, first):
    size = lax.axis_size(axis)
    members = [(first + j) % size for j in range(size)]
    return lax.all_to_all(x, axis, 0, 0, axis_index_groups=[members], tiled=True)


def dot(a, b, ca, cb):
    return lax.dot_general(a, b, (((ca,), (cb,)), ((), ())), preferred_element_type=F32)


def div(x, n):
    return lax.shift_right_logical(x, jnp.int32(n.bit_length() - 1))


def mod(x, n):
    return x & (n - 1)


def one_hot(ref, of_row, of_column):
    rows, columns = ref.shape
    r = of_row(lax.broadcasted_iota(jnp.int32, (rows, 128), 0))
    c = of_column(lax.broadcasted_iota(jnp.int32, (1, columns), 1))
    same = jnp.concatenate([r] * (columns // 128), axis=1) == c
    ref[...] = jnp.where(same, 1.0, 0.0).astype(BF16)


class Plan:
    def __init__(self, groups, n_dp, held):
        self.groups, self.n_dp, self.held = groups, n_dp, held
        self.owned = NB // groups
        self.width = self.owned * BS
        self.line = self.owned * held
        assert all(n & (n - 1) == 0 for n in (groups, n_dp, held))

    def peer_m(self, r):
        return mod(div(r, self.held), self.owned)

    def peer_i(self, r):
        high = div(mod(r, self.owned * self.owned), self.line)
        return high * self.held + mod(r, self.held)

    def target(self, r):
        peer = mod(div(r, self.owned * self.owned) + MP_FIRST, self.groups)
        return peer * self.owned + self.peer_m(r)

    def feature(self, r, first):
        member = mod(div(r, self.line) + first, self.n_dp)
        return div(mod(r, self.line), self.held) * BS + member * self.held + mod(r, self.held)

    def turn(self, x, first, back):
        by = (MP_FIRST * self.owned * self.owned - first * self.line) % self.width
        by = self.width - by if back else by
        return jnp.concatenate([x[by:], x[:by]], axis=0) if by % self.width else x


def load_kernel(plan, right, left, copies, spread, unspread, tiles, features, block, m, r, l, sems):
    loads = [pltpu.make_async_copy(right, r, sems.at[0]), pltpu.make_async_copy(left, l, sems.at[1])]
    for load in loads:
        load.start()
    one_hot(spread, plan.target, lambda c: c)
    one_hot(unspread, lambda n: n, plan.target)
    one_hot(tiles, lambda n: n, lambda c: mod(c, BS) + BS)
    one_hot(features, lambda n: plan.feature(n, DP_FIRST), lambda c: c)
    one_hot(block, plan.peer_i, lambda c: div(c, BS))
    one_hot(m, plan.peer_m, lambda c: div(c, BS))
    for load in loads:
        load.wait()
    copies[...] = jnp.broadcast_to(jnp.concatenate([r[...], l[...]], axis=2), copies.shape)


def first_kernel(plan, lines, spread, tiles, features, block, m, right, left):
    some = dot(spread[...], lines[...], 1, 1).astype(BF16)
    right[...] = dot(some, features[...], 1, 0).astype(BF16) * block[...]
    turned = plan.turn(lines[...], DP_FIRST, False)
    left[...] = (dot(turned, tiles[...], 1, 0) * 0.5).astype(BF16) * m[...]


def middle_kernel(plan, left, inner, cotangent, tiles, m, dmixed, part_left, activated, act, pres, dpres, sems):
    steps, copies = len(STEPS), []
    spans = [pl.ds(sum(STEPS[:s]), STEPS[s]) for s in range(steps)]

    def pre_of(s):
        pres[spans[s], :] = dot(inner[:, spans[s]], left[...], 0, 0)

    def slope_of(s):
        at = spans[s]
        half = pres[at, :]
        twice_cdf = 1.0 + lax.erf(half * 1.4142135623730951)
        act[at, :] = (half * twice_cdf).astype(BF16)
        density = jnp.exp2(half * half * -2.8853900817779268) * 1.5957691216057308
        slope = twice_cdf + half * density
        dpres[at, :] = (cotangent[at, :].astype(F32) * slope).astype(BF16)

    def products_of(s, total):
        at = spans[s]
        dmixed[:, at] = dot(left[...], dpres[at, :], 1, 1).astype(BF16)
        part = dot(inner[:, at], dpres[at, :], 1, 0)
        return part if total is None else total + part

    total = None
    pre_of(0)
    for s in range(steps):
        if s + 1 < steps:
            pre_of(s + 1)
        slope_of(s)
        if s:
            total = products_of(s - 1, total)
        at = spans[s]
        copies.append(pltpu.make_async_copy(act.at[at, :], activated.at[at, :], sems.at[s]))
        copies[-1].start()
    total = products_of(steps - 1, total)
    part = (total * 0.5).astype(BF16) * m[...]
    part_left[...] = plan.turn(dot(part, tiles[...], 1, 1), DP_FIRST, True).astype(BF16)
    for copy in copies:
        copy.wait()


def last_kernel(plan, part, part_left, unspread, features, parts):
    part = dot(unspread[...], part[...], 1, 0).astype(BF16)
    parts[...] = (dot(features[...], part, 1, 1) + part_left[...].astype(F32)).astype(BF16)


HBM = pl.BlockSpec(memory_space=pltpu.HBM)
VMEM = pl.BlockSpec(memory_space=pltpu.VMEM)


def call(kernel, inputs, outputs, scratch=(), hbm_in=False, hbm_out=(), limit=24):
    outs = tuple(
        jax.ShapeDtypeStruct(shape, BF16) if k in hbm_out else pltpu.VMEM(shape, BF16)
        for k, shape in enumerate(outputs)
    )
    return pl.pallas_call(
        kernel,
        out_shape=outs,
        in_specs=[HBM if hbm_in else VMEM] * len(inputs),
        out_specs=tuple(HBM if k in hbm_out else VMEM for k in range(len(outs))),
        scratch_shapes=scratch,
        compiler_params=pltpu.CompilerParams(vmem_limit_bytes=limit * 1024 * 1024),
    )(*inputs)


def shards(tokens, right_weight, left_weight, cotangent):
    rows = tokens.shape[0]
    groups, n_dp = lax.axis_size("mp"), lax.axis_size("dp")
    plan = Plan(groups, n_dp, right_weight.shape[1])
    width = plan.width
    line = (*right_weight.shape[:2], 2 * BS)
    square, tall, wide = (width, width), (width, 2 * BS), (2 * BS, width)

    copies, spread, unspread, tiles, features, block, m = call(
        functools.partial(load_kernel, plan),
        (right_weight, left_weight),
        ((n_dp, *line), tall, wide, wide, square, square, square),
        scratch=[
            pltpu.VMEM(right_weight.shape, BF16),
            pltpu.VMEM(left_weight.shape, BF16),
            pltpu.SemaphoreType.DMA((2,)),
        ],
        hbm_in=True,
        limit=60,
    )
    lines = exchange(copies, "dp", DP_FIRST).reshape(tall)

    right, left = call(
        functools.partial(first_kernel, plan),
        (lines, spread, tiles, features, block, m),
        (square, square),
    )
    inner = dot(right, tokens, 1, 1).astype(BF16)
    inner = exchange(inner.reshape(groups, -1, rows), "mp", MP_FIRST).reshape(width, rows)

    dmixed, part_left, activated = call(
        functools.partial(middle_kernel, plan),
        (left, inner, cotangent, tiles, m),
        ((width, rows), tall, (rows, width)),
        scratch=[
            pltpu.VMEM((rows, width), BF16),
            pltpu.VMEM((rows, width), F32),
            pltpu.VMEM((rows, width), BF16),
            pltpu.SemaphoreType.DMA((len(STEPS),)),
        ],
        hbm_out=(2,),
    )
    dinner = exchange(dmixed.reshape(groups, -1, rows), "mp", MP_FIRST).reshape(width, rows)

    part = dot(dinner, tokens, 1, 0).astype(BF16) * block
    (parts,) = call(
        functools.partial(last_kernel, plan),
        (part, part_left, unspread, features),
        (tall,),
    )
    parts = exchange(parts.reshape(n_dp, *line), "dp", DP_FIRST)
    right = jnp.sum(parts[..., :BS].astype(F32), axis=0)
    left = jnp.sum(parts[..., BS:].astype(F32), axis=0)
    return (activated, right, left)


def solution(mesh):
    return jax.shard_map(
        shards,
        mesh=mesh,
        in_specs=(P("dp", "mp"), P("mp", "dp", None), P("mp", "dp", None), P("dp", "mp")),
        out_specs=(P("dp", "mp"), P("mp", "dp", None), P("mp", "dp", None)),
        check_vma=False,
    )
```

```python
import functools

import jax
import jax.numpy as jnp
from jax import lax
from jax.experimental import pallas as pl
from jax.experimental.pallas import tpu as pltpu
from jax.sharding import PartitionSpec as P

NB = 64
BS = 64
F32, BF16 = jnp.float32, jnp.bfloat16
DP_FIRST = 24
MP_FIRST = 9
STEPS = (256, 512, 256)


def exchange(x, axis, first):
    size = lax.axis_size(axis)
    members = [(first + j) % size for j in range(size)]
    return lax.all_to_all(x, axis, 0, 0, axis_index_groups=[members], tiled=True)


def dot(a, b, ca, cb):
    return lax.dot_general(a, b, (((ca,), (cb,)), ((), ())), preferred_element_type=F32)


def div(x, n):
    return lax.shift_right_logical(x, jnp.int32(n.bit_length() - 1))


def mod(x, n):
    return x & (n - 1)


def one_hot(ref, of_row, of_column):
    rows, columns = ref.shape
    r = of_row(lax.broadcasted_iota(jnp.int32, (rows, 128), 0))
    c = of_column(lax.broadcasted_iota(jnp.int32, (1, columns), 1))
    same = jnp.concatenate([r] * (columns // 128), axis=1) == c
    ref[...] = jnp.where(same, 1.0, 0.0).astype(BF16)


class Plan:
    def __init__(self, groups, n_dp, held):
        self.groups, self.n_dp, self.held = groups, n_dp, held
        self.owned = NB // groups
        self.width = self.owned * BS
        self.line = self.owned * held
        assert all(n & (n - 1) == 0 for n in (groups, n_dp, held))

    def peer_m(self, r):
        return mod(div(r, self.held), self.owned)

    def peer_i(self, r):
        high = div(mod(r, self.owned * self.owned), self.line)
        return high * self.held + mod(r, self.held)

    def target(self, r):
        peer = mod(div(r, self.owned * self.owned) + MP_FIRST, self.groups)
        return peer * self.owned + self.peer_m(r)

    def feature(self, r, first):
        member = mod(div(r, self.line) + first, self.n_dp)
        return div(mod(r, self.line), self.held) * BS + member * self.held + mod(r, self.held)

    def turn(self, x, first, back):
        by = (MP_FIRST * self.owned * self.owned - first * self.line) % self.width
        by = self.width - by if back else by
        return jnp.concatenate([x[by:], x[:by]], axis=0) if by % self.width else x


def load_kernel(plan, right, left, copies, spread, unspread, tiles, features, block, m, r, l, sems):
    loads = [pltpu.make_async_copy(right, r, sems.at[0]), pltpu.make_async_copy(left, l, sems.at[1])]
    for load in loads:
        load.start()
    one_hot(spread, plan.target, lambda c: c)
    one_hot(unspread, lambda n: n, plan.target)
    one_hot(tiles, lambda n: n, lambda c: mod(c, BS) + BS)
    one_hot(features, lambda n: plan.feature(n, DP_FIRST), lambda c: c)
    one_hot(block, plan.peer_i, lambda c: div(c, BS))
    one_hot(m, plan.peer_m, lambda c: div(c, BS))
    for load in loads:
        load.wait()
    copies[...] = jnp.broadcast_to(jnp.concatenate([r[...], l[...]], axis=2), copies.shape)


def first_kernel(plan, lines, spread, tiles, features, block, m, right, left):
    some = dot(spread[...], lines[...], 1, 1).astype(BF16)
    right[...] = dot(some, features[...], 1, 0).astype(BF16) * block[...]
    turned = plan.turn(lines[...], DP_FIRST, False)
    left[...] = (dot(turned, tiles[...], 1, 0) * 0.5).astype(BF16) * m[...]


def middle_kernel(plan, left, inner, cotangent, tiles, m, dmixed, part_left, activated, act, pres, dpres, sems):
    steps, copies = len(STEPS), []
    spans = [pl.ds(sum(STEPS[:s]), STEPS[s]) for s in range(steps)]

    def pre_of(s):
        pres[spans[s], :] = dot(inner[:, spans[s]], left[...], 0, 0)

    def slope_of(s):
        at = spans[s]
        half = pres[at, :]
        twice_cdf = 1.0 + lax.erf(half * 1.4142135623730951)
        act[at, :] = (half * twice_cdf).astype(BF16)
        density = jnp.exp2(half * half * -2.8853900817779268) * 1.5957691216057308
        slope = twice_cdf + half * density
        dpres[at, :] = (cotangent[at, :].astype(F32) * slope).astype(BF16)

    def products_of(s, total):
        at = spans[s]
        dmixed[:, at] = dot(left[...], dpres[at, :], 1, 1).astype(BF16)
        part = dot(inner[:, at], dpres[at, :], 1, 0)
        return part if total is None else total + part

    total = None
    pre_of(0)
    for s in range(steps):
        if s + 1 < steps:
            pre_of(s + 1)
        slope_of(s)
        if s:
            total = products_of(s - 1, total)
        at = spans[s]
        copies.append(pltpu.make_async_copy(act.at[at, :], activated.at[at, :], sems.at[s]))
        copies[-1].start()
    total = products_of(steps - 1, total)
    part = (total * 0.5).astype(BF16) * m[...]
    part_left[...] = plan.turn(dot(part, tiles[...], 1, 1), DP_FIRST, True).astype(BF16)
    for copy in copies:
        copy.wait()


HBM = pl.BlockSpec(memory_space=pltpu.HBM)
VMEM = pl.BlockSpec(memory_space=pltpu.VMEM)


def call(kernel, inputs, outputs, scratch=(), hbm_in=False, hbm_out=(), limit=24):
    outs = tuple(
        jax.ShapeDtypeStruct(shape, BF16) if k in hbm_out else pltpu.VMEM(shape, BF16)
        for k, shape in enumerate(outputs)
    )
    return pl.pallas_call(
        kernel,
        out_shape=outs,
        in_specs=[HBM if hbm_in else VMEM] * len(inputs),
        out_specs=tuple(HBM if k in hbm_out else VMEM for k in range(len(outs))),
        scratch_shapes=scratch,
        compiler_params=pltpu.CompilerParams(vmem_limit_bytes=limit * 1024 * 1024),
    )(*inputs)


def shards(tokens, right_weight, left_weight, cotangent):
    rows = tokens.shape[0]
    groups, n_dp = lax.axis_size("mp"), lax.axis_size("dp")
    plan = Plan(groups, n_dp, right_weight.shape[1])
    width = plan.width
    line = (*right_weight.shape[:2], 2 * BS)
    square, tall, wide = (width, width), (width, 2 * BS), (2 * BS, width)

    copies, spread, unspread, tiles, features, block, m = call(
        functools.partial(load_kernel, plan),
        (right_weight, left_weight),
        ((n_dp, *line), tall, wide, wide, square, square, square),
        scratch=[
            pltpu.VMEM(right_weight.shape, BF16),
            pltpu.VMEM(left_weight.shape, BF16),
            pltpu.SemaphoreType.DMA((2,)),
        ],
        hbm_in=True,
        limit=60,
    )
    lines = exchange(copies, "dp", DP_FIRST).reshape(tall)

    right, left = call(
        functools.partial(first_kernel, plan),
        (lines, spread, tiles, features, block, m),
        (square, square),
    )
    inner = dot(right, tokens, 1, 1).astype(BF16)
    inner = exchange(inner.reshape(groups, -1, rows), "mp", MP_FIRST).reshape(width, rows)

    dmixed, part_left, activated = call(
        functools.partial(middle_kernel, plan),
        (left, inner, cotangent, tiles, m),
        ((width, rows), tall, (rows, width)),
        scratch=[
            pltpu.VMEM((rows, width), BF16),
            pltpu.VMEM((rows, width), F32),
            pltpu.VMEM((rows, width), BF16),
            pltpu.SemaphoreType.DMA((len(STEPS),)),
        ],
        hbm_out=(2,),
    )
    dinner = exchange(dmixed.reshape(groups, -1, rows), "mp", MP_FIRST).reshape(width, rows)

    part = dot(dinner, tokens, 1, 0).astype(BF16) * block
    part = dot(unspread, part, 1, 0).astype(BF16)
    parts = (dot(features, part, 1, 1) + part_left.astype(F32)).astype(BF16)
    parts = exchange(parts.reshape(n_dp, *line), "dp", DP_FIRST)
    right = jnp.sum(parts[..., :BS].astype(F32), axis=0)
    left = jnp.sum(parts[..., BS:].astype(F32), axis=0)
    return (activated, right, left)


def solution(mesh):
    return jax.shard_map(
        shards,
        mesh=mesh,
        in_specs=(P("dp", "mp"), P("mp", "dp", None), P("mp", "dp", None), P("dp", "mp")),
        out_specs=(P("dp", "mp"), P("mp", "dp", None), P("mp", "dp", None)),
        check_vma=False,
    )
```

```python
import functools

import jax
import jax.numpy as jnp
from jax import lax
from jax.experimental import pallas as pl
from jax.experimental.pallas import tpu as pltpu
from jax.sharding import PartitionSpec as P

NB = 64
BS = 64
F32, BF16 = jnp.float32, jnp.bfloat16
WEIGHTS_FIRST = 26
GRADS_FIRST = 24
MP_FIRST = 9
STEPS = (256, 512, 256)


def exchange(x, axis, first):
    size = lax.axis_size(axis)
    members = [(first + j) % size for j in range(size)]
    return lax.all_to_all(x, axis, 0, 0, axis_index_groups=[members], tiled=True)


def dot(a, b, ca, cb):
    return lax.dot_general(a, b, (((ca,), (cb,)), ((), ())), preferred_element_type=F32)


def div(x, n):
    return lax.shift_right_logical(x, jnp.int32(n.bit_length() - 1))


def mod(x, n):
    return x & (n - 1)


def one_hot(ref, of_row, of_column):
    rows, columns = ref.shape
    r = of_row(lax.broadcasted_iota(jnp.int32, (rows, 128), 0))
    c = of_column(lax.broadcasted_iota(jnp.int32, (1, columns), 1))
    same = jnp.concatenate([r] * (columns // 128), axis=1) == c
    ref[...] = jnp.where(same, 1.0, 0.0).astype(BF16)


class Plan:
    def __init__(self, groups, n_dp, held):
        self.groups, self.n_dp, self.held = groups, n_dp, held
        self.owned = NB // groups
        self.width = self.owned * BS
        self.line = self.owned * held
        assert all(n & (n - 1) == 0 for n in (groups, n_dp, held))

    def peer_m(self, r):
        return mod(div(r, self.held), self.owned)

    def peer_i(self, r):
        high = div(mod(r, self.owned * self.owned), self.line)
        return high * self.held + mod(r, self.held)

    def target(self, r):
        peer = mod(div(r, self.owned * self.owned) + MP_FIRST, self.groups)
        return peer * self.owned + self.peer_m(r)

    def feature(self, r, first):
        member = mod(div(r, self.line) + first, self.n_dp)
        return div(mod(r, self.line), self.held) * BS + member * self.held + mod(r, self.held)

    def turn(self, x, first, back):
        by = (MP_FIRST * self.owned * self.owned - first * self.line) % self.width
        by = self.width - by if back else by
        return jnp.concatenate([x[by:], x[:by]], axis=0) if by % self.width else x


def load_kernel(plan, right, left, copies, spread, unspread, tiles, wfeatures, gfeatures, block, m, r, l, sems):
    loads = [pltpu.make_async_copy(right, r, sems.at[0]), pltpu.make_async_copy(left, l, sems.at[1])]
    for load in loads:
        load.start()
    one_hot(spread, plan.target, lambda c: c)
    one_hot(unspread, lambda n: n, plan.target)
    one_hot(tiles, lambda n: n, lambda c: mod(c, BS) + BS)
    one_hot(wfeatures, lambda n: plan.feature(n, WEIGHTS_FIRST), lambda c: c)
    one_hot(gfeatures, lambda n: plan.feature(n, GRADS_FIRST), lambda c: c)
    one_hot(block, plan.peer_i, lambda c: div(c, BS))
    one_hot(m, plan.peer_m, lambda c: div(c, BS))
    for load in loads:
        load.wait()
    copies[...] = jnp.broadcast_to(jnp.concatenate([r[...], l[...]], axis=2), copies.shape)


def first_kernel(plan, lines, spread, tiles, features, block, m, right, left):
    some = dot(spread[...], lines[...], 1, 1).astype(BF16)
    right[...] = dot(some, features[...], 1, 0).astype(BF16) * block[...]
    turned = plan.turn(lines[...], WEIGHTS_FIRST, False)
    left[...] = (dot(turned, tiles[...], 1, 0) * 0.5).astype(BF16) * m[...]


def middle_kernel(left, inner, cotangent, dmixed, part_left, activated, act, pres, dpres, sems):
    steps, copies = len(STEPS), []
    spans = [pl.ds(sum(STEPS[:s]), STEPS[s]) for s in range(steps)]

    def pre_of(s):
        pres[spans[s], :] = dot(inner[:, spans[s]], left[...], 0, 0)

    def slope_of(s):
        at = spans[s]
        half = pres[at, :]
        twice_cdf = 1.0 + lax.erf(half * 1.4142135623730951)
        act[at, :] = (half * twice_cdf).astype(BF16)
        density = jnp.exp2(half * half * -2.8853900817779268) * 1.5957691216057308
        slope = twice_cdf + half * density
        dpres[at, :] = (cotangent[at, :].astype(F32) * slope).astype(BF16)

    def products_of(s, total):
        at = spans[s]
        dmixed[:, at] = dot(left[...], dpres[at, :], 1, 1).astype(BF16)
        part = dot(inner[:, at], dpres[at, :], 1, 0)
        return part if total is None else total + part

    total = None
    pre_of(0)
    for s in range(steps):
        if s + 1 < steps:
            pre_of(s + 1)
        slope_of(s)
        if s:
            total = products_of(s - 1, total)
        at = spans[s]
        copies.append(pltpu.make_async_copy(act.at[at, :], activated.at[at, :], sems.at[s]))
        copies[-1].start()
    total = products_of(steps - 1, total)
    part_left[...] = (total * 0.5).astype(BF16)
    for copy in copies:
        copy.wait()


def last_kernel(plan, part, part_left, unspread, features, tiles, m, parts):
    left = plan.turn(dot(part_left[...] * m[...], tiles[...], 1, 1), GRADS_FIRST, True)
    part = dot(unspread[...], part[...], 1, 0).astype(BF16)
    parts[...] = (dot(features[...], part, 1, 1) + left).astype(BF16)


HBM = pl.BlockSpec(memory_space=pltpu.HBM)
VMEM = pl.BlockSpec(memory_space=pltpu.VMEM)


def call(kernel, inputs, outputs, scratch=(), hbm_in=False, hbm_out=(), limit=24):
    outs = tuple(
        jax.ShapeDtypeStruct(shape, BF16) if k in hbm_out else pltpu.VMEM(shape, BF16)
        for k, shape in enumerate(outputs)
    )
    return pl.pallas_call(
        kernel,
        out_shape=outs,
        in_specs=[HBM if hbm_in else VMEM] * len(inputs),
        out_specs=tuple(HBM if k in hbm_out else VMEM for k in range(len(outs))),
        scratch_shapes=scratch,
        compiler_params=pltpu.CompilerParams(vmem_limit_bytes=limit * 1024 * 1024),
    )(*inputs)


def shards(tokens, right_weight, left_weight, cotangent):
    rows = tokens.shape[0]
    groups, n_dp = lax.axis_size("mp"), lax.axis_size("dp")
    plan = Plan(groups, n_dp, right_weight.shape[1])
    width = plan.width
    line = (*right_weight.shape[:2], 2 * BS)
    square, tall, wide = (width, width), (width, 2 * BS), (2 * BS, width)

    copies, spread, unspread, tiles, wfeatures, gfeatures, block, m = call(
        functools.partial(load_kernel, plan),
        (right_weight, left_weight),
        ((n_dp, *line), tall, wide, wide, square, square, square, square),
        scratch=[
            pltpu.VMEM(right_weight.shape, BF16),
            pltpu.VMEM(left_weight.shape, BF16),
            pltpu.SemaphoreType.DMA((2,)),
        ],
        hbm_in=True,
        limit=60,
    )
    lines = exchange(copies, "dp", WEIGHTS_FIRST).reshape(tall)

    right, left = call(
        functools.partial(first_kernel, plan),
        (lines, spread, tiles, wfeatures, block, m),
        (square, square),
    )
    inner = dot(right, tokens, 1, 1).astype(BF16)
    inner = exchange(inner.reshape(groups, -1, rows), "mp", MP_FIRST).reshape(width, rows)

    dmixed, part_left, activated = call(
        middle_kernel,
        (left, inner, cotangent),
        ((width, rows), square, (rows, width)),
        scratch=[
            pltpu.VMEM((rows, width), BF16),
            pltpu.VMEM((rows, width), F32),
            pltpu.VMEM((rows, width), BF16),
            pltpu.SemaphoreType.DMA((len(STEPS),)),
        ],
        hbm_out=(2,),
    )
    dinner = exchange(dmixed.reshape(groups, -1, rows), "mp", MP_FIRST).reshape(width, rows)

    part = dot(dinner, tokens, 1, 0).astype(BF16) * block
    (parts,) = call(
        functools.partial(last_kernel, plan),
        (part, part_left, unspread, gfeatures, tiles, m),
        (tall,),
    )
    sums = jnp.sum(exchange(parts.reshape(n_dp, *line), "dp", GRADS_FIRST).astype(F32), axis=0)
    return (activated, sums[..., :BS], sums[..., BS:])


def solution(mesh):
    return jax.shard_map(
        shards,
        mesh=mesh,
        in_specs=(P("dp", "mp"), P("mp", "dp", None), P("mp", "dp", None), P("dp", "mp")),
        out_specs=(P("dp", "mp"), P("mp", "dp", None), P("mp", "dp", None)),
        check_vma=False,
    )
```
